32 devices in a mesh: src: 4 (over z), rcv: 8 (over y, x, core).
Axes of the slice: x: 2, y: 2, z: 4, core: 2. Of those that a mesh axis runs over, the one named last changes fastest.
Arguments:
- traces: bfloat16 [512, 2048, 512], P('src', 'rcv'), may hold values from -6 to 6
- virtual_source_index: int32 [256], replicated, may hold values from 0 to 2047
Outputs:
- correlations: float32 [256, 2048, 512], P('rcv', 'src')
The draws below stay inside these ranges and needn't reach their ends.
Inputs may be any that keep to these rules, and one draw needn't show every extreme that they name: `virtual_source_index`: receiver numbers; a receiver may be listed more than once.
All inputs are finite; a program needn't handle non-finite values.
Results may differ from the reference program's by a relative error of at most 0.0064.
Values may be sent and summed in bfloat16 or wider, within the bound.
A program may use at most 192 MiB of HBM per device.

```python
import math
import jax
import jax.numpy as jnp
from jax import lax

NT = 512
NF = 128
RCV = 2048
VS = 256
SHOTS = 512


def place_ends(array, stream_key, smallest, top_value):
    dims = array.shape
    place = [jax.random.randint(jax.random.fold_in(stream_key, axis), (), 0, dims[axis]) for axis in range(len(dims))]
    array = array.at[tuple(place)].set(smallest)
    longest = dims.index(max(dims))
    place[longest] = (place[longest] + 1) % dims[longest]
    return array.at[tuple(place)].set(top_value)


def shard_levels(key, dims, pieces, least, high):
    loudness = 1.0
    for position, shards_of in pieces:
        steps = jax.random.uniform(jax.random.fold_in(jax.random.fold_in(key, 6), position), (shards_of,), jnp.float32, least / len(pieces), high / len(pieces))
        loudness = loudness * jnp.repeat(jnp.exp(steps), dims[position] // shards_of).reshape((-1,) + (1,) * (len(dims) - 1 - position))
    return loudness


def noise(own_key, shape, width, most, split=(), kind=jnp.bfloat16):
    entries = jax.random.normal(own_key, shape, jnp.float32) * width
    if len(split) > 0:
        entries = shard_levels(own_key, shape, split, -0.22, 0.18) * entries
    return jnp.clip(entries, min=-most, max=most).astype(kind)


def setup_inputs(seed: int = 0) -> dict:
    streams_of = jax.random.split(jax.random.key(seed), 3)
    return {
        "traces": noise(streams_of[0], (SHOTS, RCV, NT), 1.0, 6.0, ((0, 4), (1, 8))),
        "virtual_source_index": place_ends(jax.random.randint(streams_of[1], (VS,), 0, RCV), jax.random.fold_in(streams_of[1], 1), 0, RCV - 1).astype(jnp.int32),
    }


def make_tables():
    freqs = jnp.arange(NF, dtype=jnp.int32)
    times = jnp.arange(NT, dtype=jnp.int32)
    phase = (freqs[:, None] * times[None, :] % NT).astype(jnp.float32) * (2.0 * math.pi / NT)
    basis = jnp.stack([jnp.cos(phase), -jnp.sin(phase)], axis=1)
    forward = (basis / jnp.sqrt(jnp.float32(NT))).astype(jnp.bfloat16)
    inverse = (basis / jnp.sqrt(jnp.float32(NF))).astype(jnp.bfloat16)
    return (forward, inverse)

def complex_gram(left_operand, right_operand):
    high_precision = lax.Precision.HIGHEST
    real_part = jnp.einsum('ekg,ekh->egh', left_operand[:, 0], right_operand[:, 0], precision=high_precision) + jnp.einsum('ekg,ekh->egh', left_operand[:, 1], right_operand[:, 1], precision=high_precision)
    imaginary_part = jnp.einsum('ekg,ekh->egh', left_operand[:, 0], right_operand[:, 1], precision=high_precision) - jnp.einsum('ekg,ekh->egh', left_operand[:, 1], right_operand[:, 0], precision=high_precision)
    return jnp.stack([real_part, imaginary_part], axis=1)

def reference(traces, virtual_source_index):
    forward, inverse = make_tables()
    frequency_block = 8
    flat = traces.reshape(SHOTS * RCV, NT)
    scale = 1.0 / jnp.sqrt(jnp.float32(SHOTS))

    def one_block(table):
        spec = jnp.dot(flat, table.reshape(frequency_block * 2, NT).T, preferred_element_type=jnp.float32)
        spec = spec.astype(jnp.bfloat16).reshape(SHOTS, RCV, frequency_block, 2).transpose(2, 3, 0, 1).astype(jnp.float32)
        rows = jnp.take(spec, virtual_source_index, axis=3)
        gram = complex_gram(rows, spec) * scale
        return gram.astype(jnp.bfloat16)
    scaled = lax.map(one_block, forward.reshape(NF // frequency_block, frequency_block, 2, NT))
    scaled = scaled.reshape(NF, 2, VS, RCV).transpose(2, 0, 1, 3)
    inverse_flattened = inverse.reshape(2 * NF, NT)

    def one_source(block):
        return jnp.dot(block.reshape(2 * NF, RCV).T, inverse_flattened, preferred_element_type=jnp.float32)
    return lax.map(one_source, scaled)
```

```python
import functools
import math

import jax
import jax.numpy as jnp
from jax import lax
from jax.experimental import pallas as pl
from jax.experimental.pallas import tpu as pltpu
from jax.sharding import PartitionSpec as P

NF = 128
AHEAD = 3
LAG = 3
VMEM_LIMIT = 62 * 2**20
MESH = pl.DeviceIdType.MESH


def make_tables(times_count):
    freqs = jnp.arange(NF, dtype=jnp.int32)
    times = jnp.arange(times_count, dtype=jnp.int32)
    phase = (freqs[:, None] * times[None, :] % times_count).astype(jnp.float32) * (
        2.0 * math.pi / times_count
    )
    basis = jnp.stack([jnp.cos(phase), -jnp.sin(phase)], axis=1)
    forward = (basis / jnp.sqrt(jnp.float32(times_count))).astype(jnp.bfloat16)
    inverse = (basis / jnp.sqrt(jnp.float32(NF))).astype(jnp.bfloat16)
    return (
        forward.reshape(2 * NF, times_count),
        inverse.reshape(2 * NF, times_count),
    )


def forward_kernel(table_ref, traces_ref, out_ref):
    shots, receivers, times_count = traces_ref.shape
    spectra = lax.dot_general(
        table_ref[...],
        traces_ref[...].reshape(shots * receivers, times_count),
        (((1,), (1,)), ((), ())),
        preferred_element_type=jnp.float32,
    )
    out_ref[...] = spectra.reshape(out_ref.shape).astype(out_ref.dtype)


def forward_transform(table, traces):
    shots, receivers, times_count = traces.shape
    rows = table.shape[0]
    block = math.gcd(shots, 16)
    return pl.pallas_call(
        forward_kernel,
        grid=(shots // block,),
        in_specs=[
            pl.BlockSpec((rows, times_count), lambda i: (0, 0)),
            pl.BlockSpec((block, receivers, times_count), lambda i: (i, 0, 0)),
        ],
        out_specs=pl.BlockSpec((rows, block, receivers), lambda i: (0, i, 0)),
        out_shape=jax.ShapeDtypeStruct((rows, shots, receivers), jnp.bfloat16),
        compiler_params=pltpu.CompilerParams(vmem_limit_bytes=VMEM_LIMIT),
        cost_estimate=pl.CostEstimate(
            flops=2 * rows * traces.size, bytes_accessed=4 * traces.size, transcendentals=0
        ),
    )(table, traces)


def inverse_kernel(folded_ref, table_ref, out_ref):
    rows, sources, receivers = folded_ref.shape
    lags = lax.dot_general(
        folded_ref[...].reshape(rows, sources * receivers),
        table_ref[...],
        (((0,), (0,)), ((), ())),
        preferred_element_type=jnp.float32,
    )
    out_ref[...] = lags.reshape(out_ref.shape)


def inverse_transform(folded, table):
    rows, sources, receivers = folded.shape
    times_count = table.shape[1]
    block = math.gcd(receivers, 128)
    return pl.pallas_call(
        inverse_kernel,
        grid=(receivers // block,),
        in_specs=[
            pl.BlockSpec((rows, sources, block), lambda i: (0, 0, i)),
            pl.BlockSpec((rows, times_count), lambda i: (0, 0)),
        ],
        out_specs=pl.BlockSpec((sources, block, times_count), lambda i: (0, i, 0)),
        out_shape=jax.ShapeDtypeStruct((sources, receivers, times_count), jnp.float32),
        compiler_params=pltpu.CompilerParams(vmem_limit_bytes=VMEM_LIMIT),
        cost_estimate=pl.CostEstimate(
            flops=2 * folded.size * times_count,
            bytes_accessed=4 * sources * receivers * times_count,
            transcendentals=0,
        ),
    )(folded, table)


def exchange_kernel(
    scale,
    spectra,
    pick,
    folded,
    sbuf,
    xbuf,
    hbuf,
    hrows,
    psend,
    pbuf,
    acc,
    fsend,
    r_send,
    r_recv,
    r_own,
    h_send,
    h_recv,
    p_send,
    p_recv,
    w_send,
    w_recv,
    w_own,
):
    chunks, n_rcv, _, shots, width = sbuf.shape
    _, _, _, sources, receivers = psend.shape
    n_src = lax.axis_size("src")
    half = n_src // 2
    share = hbuf.shape[2] - 1
    blocks = n_rcv // n_src
    own = sources // n_rcv
    j = lax.axis_index("rcv")
    m = lax.axis_index("src")
    side = m // half
    depth = (1 - side) * (half - 1 - m) + side * (m - half)
    handles = depth * share < half

    def place(which, at):
        return (1 - which) * (half - 1 - at) + which * (half + at)

    def r_copy(i, o):
        peer = lax.rem(j + o, n_rcv)
        return pltpu.make_async_remote_copy(
            src_ref=spectra.at[peer, i],
            dst_ref=sbuf.at[i, j],
            send_sem=r_send.at[i, o - 1],
            recv_sem=r_recv.at[i, o - 1],
            device_id={"rcv": peer},
            device_id_type=MESH,
        )

    def r_arrival(i, o):
        peer = lax.rem(j + n_rcv - o, n_rcv)
        return pltpu.make_async_remote_copy(
            src_ref=spectra.at[peer, i],
            dst_ref=sbuf.at[i, peer],
            send_sem=r_send.at[i, o - 1],
            recv_sem=r_recv.at[i, o - 1],
            device_id={"rcv": peer},
            device_id_type=MESH,
        )

    def r_local(i):
        return pltpu.make_async_copy(spectra.at[j, i], sbuf.at[i, j], r_own.at[i])

    def h_copy(i, o, src, dst, which):
        at = lax.rem(depth + o, half)
        return pltpu.make_async_remote_copy(
            src_ref=src,
            dst_ref=dst,
            send_sem=h_send.at[i, o - 1, which],
            recv_sem=h_recv.at[i, o - 1, which],
            device_id={"src": place(side, at)},
            device_id_type=MESH,
        )

    def piece(i, block):
        return sbuf.at[i, pl.ds(block * blocks, blocks)]

    def h_rows(i, o):
        return h_copy(i, o, xbuf.at[i], hrows.at[i, o - 1], 0)

    def h_far(i, o, u):
        at = lax.rem(depth + o, half)
        block = place(1 - side, lax.rem(at * share + u, half))
        return h_copy(i, o, piece(i, block), hbuf.at[i, o - 1, 1 + u], 1 + u)

    def h_near(i, o):
        at = lax.rem(depth + o, half)
        return h_copy(i, o, piece(i, place(side, at)), hbuf.at[i, o - 1, 0], 1 + share)

    def p_copy(i, u):
        slot = lax.rem(i, 2)
        target = place(1 - side, lax.rem(depth * share + u, half))
        return pltpu.make_async_remote_copy(
            src_ref=psend.at[slot, u],
            dst_ref=pbuf.at[i],
            send_sem=p_send.at[slot, u],
            recv_sem=p_recv.at[i],
            device_id={"src": target},
            device_id_type=MESH,
        )

    def w_copy(i, o):
        slot = lax.rem(i, 2)
        peer = lax.rem(j + o, n_rcv)
        return pltpu.make_async_remote_copy(
            src_ref=fsend.at[slot, peer],
            dst_ref=folded.at[j, i],
            send_sem=w_send.at[slot, o - 1],
            recv_sem=w_recv.at[i, o - 1],
            device_id={"rcv": peer},
            device_id_type=MESH,
        )

    def w_arrival(i, o):
        slot = lax.rem(i, 2)
        peer = lax.rem(j + n_rcv - o, n_rcv)
        return pltpu.make_async_remote_copy(
            src_ref=fsend.at[slot, peer],
            dst_ref=folded.at[peer, i],
            send_sem=w_send.at[slot, o - 1],
            recv_sem=w_recv.at[i, o - 1],
            device_id={"rcv": peer},
            device_id_type=MESH,
        )

    def w_local(i):
        slot = lax.rem(i, 2)
        return pltpu.make_async_copy(fsend.at[slot, j], folded.at[j, i], w_own.at[slot])

    def r_start(i):
        for o in range(1, n_rcv):
            r_copy(i, o).start()
        r_local(i).start()

    def lefts(i):
        pieces = [xbuf[i]] + [hrows[i, o - 1] for o in range(1, half)]
        real = [x.reshape(2 * shots, sources) for x in pieces]
        imaginary = [jnp.concatenate([-x[1], x[0]], axis=0) for x in pieces]
        return (real, imaginary)

    def gram(left, rights):
        total = None
        for x, y in zip(left, rights):
            part = lax.dot_general(
                x, y, (((0,), (0,)), ((), ())), preferred_element_type=jnp.float32
            )
            total = part if total is None else total + part
        return total

    def rights(i, block, which, b):
        pieces = [sbuf[i, block * blocks + b]]
        pieces += [hbuf[i, o - 1, which, b] for o in range(1, half)]
        return [y.reshape(2 * shots, width) for y in pieces]

    def gather_rows(i):
        for o in range(1, n_rcv):
            r_arrival(i, o).wait_recv()
        r_local(i).wait()
        total = None
        for owner in range(n_rcv):
            part = jnp.dot(
                sbuf[i, owner].reshape(2 * shots, width),
                pick[owner],
                preferred_element_type=jnp.float32,
            )
            total = part if total is None else total + part
        xbuf[i] = total.astype(xbuf.dtype).reshape(2, shots, sources)
        for o in range(1, half):
            h_rows(i, o).start()
            at = lax.rem(depth + o, half)

            @pl.when(at * share < half)
            def _():
                for u in range(share):
                    h_far(i, o, u).start()

            h_near(i, o).start()

    def send_partial(i):
        slot = lax.rem(i, 2)
        for o in range(1, half):
            h_rows(i, o).wait_recv()
        left = lefts(i)
        for u in range(share):
            for o in range(1, half):
                h_far(i, o, u).wait_recv()

            @pl.when(i >= 2)
            def _():
                p_copy(i, u).wait_send()

            block = place(1 - side, lax.rem(depth * share + u, half))
            for b in range(blocks):
                right = rights(i, block, 1 + u, b)
                for part in range(2):
                    psend[slot, u, part, :, b * width : (b + 1) * width] = gram(
                        left[part], right
                    ).astype(psend.dtype)
            p_copy(i, u).start()

    def finish(i):
        slot = lax.rem(i, 2)

        @pl.when(jnp.logical_not(handles))
        def _():
            for o in range(1, half):
                h_rows(i, o).wait_recv()

        for o in range(1, half):
            h_near(i, o).wait_recv()
        left = lefts(i)
        for b in range(blocks):
            right = rights(i, m, 0, b)
            for part in range(2):
                acc[part, :, b * width : (b + 1) * width] = gram(left[part], right)

        @pl.when(i >= 2)
        def _():
            for o in range(1, n_rcv):
                w_copy(i, o).wait_send()
            w_local(i).wait()

        p_arrival = p_copy(i, 0)
        p_arrival.wait_recv()
        for part in range(2):
            total = (acc[part] + pbuf[i, part].astype(jnp.float32)) * scale
            fsend[slot, :, part] = total.astype(fsend.dtype).reshape(n_rcv, own, receivers)
        for o in range(1, n_rcv):
            w_copy(i, o).start()
        w_local(i).start()

    for i in range(min(AHEAD, chunks)):
        r_start(i)

    def step(i, carry):
        @pl.when(i + AHEAD < chunks)
        def _():
            r_start(i + AHEAD)

        @pl.when(i < chunks)
        def _():
            gather_rows(i)

        @pl.when(jnp.logical_and(handles, jnp.logical_and(i >= 1, i <= chunks)))
        def _():
            send_partial(i - 1)

        @pl.when(i >= LAG)
        def _():
            finish(i - LAG)

        return carry

    lax.fori_loop(0, chunks + LAG, step, 0)

    def drain(i, carry):
        for o in range(1, n_rcv):
            r_copy(i, o).wait_send()
            w_arrival(i, o).wait_recv()
        for o in range(1, half):
            h_rows(i, o).wait_send()
            at = lax.rem(depth + o, half)

            @pl.when(at * share < half)
            def _():
                for u in range(share):
                    h_far(i, o, u).wait_send()

            h_near(i, o).wait_send()
        return carry

    lax.fori_loop(0, chunks, drain, 0)
    for i in range(max(chunks - 2, 0), chunks):

        @pl.when(handles)
        def _():
            for u in range(share):
                p_copy(i, u).wait_send()

        for o in range(1, n_rcv):
            w_copy(i, o).wait_send()
        w_local(i).wait()


def exchange(spectra, pick, n_src, all_shots):
    n_rcv, chunks, _, shots, width = spectra.shape
    sources = pick.shape[2]
    half = n_src // 2
    share = 2 if half % 2 == 0 else 1
    others = max(half - 1, 1)
    blocks = n_rcv // n_src
    receivers = blocks * width
    own = sources // n_rcv
    dma = pltpu.SemaphoreType.DMA
    kind = jnp.bfloat16
    return pl.pallas_call(
        functools.partial(exchange_kernel, 1.0 / math.sqrt(all_shots)),
        in_specs=[
            pl.BlockSpec(memory_space=pl.ANY),
            pl.BlockSpec(memory_space=pltpu.VMEM),
        ],
        out_specs=pl.BlockSpec(memory_space=pl.ANY),
        out_shape=jax.ShapeDtypeStruct((n_rcv, chunks, 2, own, receivers), kind),
        scratch_shapes=[
            pltpu.VMEM((chunks, n_rcv, 2, shots, width), kind),
            pltpu.VMEM((chunks, 2, shots, sources), kind),
            pltpu.VMEM((chunks, others, 1 + share, blocks, 2, shots, width), kind),
            pltpu.VMEM((chunks, others, 2, shots, sources), kind),
            pltpu.VMEM((2, share, 2, sources, receivers), kind),
            pltpu.VMEM((chunks, 2, sources, receivers), kind),
            pltpu.VMEM((2, sources, receivers), jnp.float32),
            pltpu.VMEM((2, n_rcv, 2, own, receivers), kind),
            dma((chunks, n_rcv - 1)),
            dma((chunks, n_rcv - 1)),
            dma((chunks,)),
            dma((chunks, others, 2 + share)),
            dma((chunks, others, 2 + share)),
            dma((2, share)),
            dma((chunks,)),
            dma((2, n_rcv - 1)),
            dma((chunks, n_rcv - 1)),
            dma((2,)),
        ],
        compiler_params=pltpu.CompilerParams(
            has_side_effects=True, vmem_limit_bytes=VMEM_LIMIT
        ),
        cost_estimate=pl.CostEstimate(
            flops=8 * chunks * all_shots * sources * receivers,
            bytes_accessed=spectra.size * 4,
            transcendentals=0,
        ),
    )(spectra, pick)


def shards(traces, virtual_source_index):
    shots, width, times_count = traces.shape
    n_src, n_rcv = lax.axis_size("src"), lax.axis_size("rcv")
    sources = virtual_source_index.shape[0]
    chunks = NF // n_rcv
    forward, inverse = make_tables(times_count)
    receivers = jnp.arange(n_rcv * width, dtype=jnp.int32)
    pick = (receivers[:, None] == virtual_source_index[None, :]).astype(jnp.bfloat16)
    pick = pick.reshape(n_rcv, width, sources)
    spectra = forward_transform(forward, traces)
    spectra = spectra.reshape(n_rcv, chunks, 2, shots, width)
    folded = exchange(spectra, pick, n_src, n_src * shots)
    folded = folded.reshape(2 * NF, folded.shape[3], folded.shape[4])
    return inverse_transform(folded, inverse)


def solution(mesh):
    placed = (P("src", "rcv", None), P())
    return jax.shard_map(
        shards, mesh=mesh, in_specs=placed, out_specs=P("rcv", "src", None), check_vma=False
    )
```
